32 devices in a mesh: row: 4 (over x, core), col: 8 (over z, y).
Axes of the slice: x: 2, y: 2, z: 4, core: 2. Of those that a mesh axis runs over, the one named last changes fastest.
Arguments:
- benefit: int32 [4096, 16384], P('row', 'col'), may hold values from 0 to 269488127, as said below
- prices: int32 [16384], P('col'), may hold values from 0 to 4095
- assignment: int32 [4096], P('row'), may hold values from -1 to 16383, as said below
- epsilon: int32 [1], replicated, may hold values from 1 to 1024
Outputs:
- new_prices: int32 [16384], P('col')
- new_assignment: int32 [4096], P('row')
The draws below stay inside these ranges and needn't reach their ends.
Inputs may be any that keep to these rules, and one draw needn't show every extreme that they name: `assignment`: each entry is -1 or an object index, and no two persons hold the same object. `benefit`: several objects may share a person's best value.
All inputs are finite; a program needn't handle non-finite values.
Results may differ from the reference program's by a relative error of at most 0.000001.
Values may be sent and summed in bfloat16 or wider, within the bound.
A program may use at most 64 MiB of HBM per device.

```python
import jax
import jax.numpy as jnp
from jax import lax

PERS_DEV = 1024
OBJ_DEV = 2048
ROUNDS = 4
PERSONS = 4096
OBJECTS = 16384


def shared_prices(key):
    return jax.random.randint(jax.random.fold_in(key, 11), (OBJECTS,), 0, 4096).astype(jnp.int32)


def draw_prices(key, part):
    return shared_prices(key)


def draw_benefit(key, part):
    price = shared_prices(key)
    tiles = OBJECTS // OBJ_DEV
    base = jax.random.randint(jax.random.fold_in(key, 12), (PERSONS, OBJECTS), 0, 268435456).astype(jnp.int32)
    tied = jax.random.randint(jax.random.fold_in(key, 13), (PERSONS,), 0, 2) == 1
    tile_one = jax.random.randint(jax.random.fold_in(key, 14), (PERSONS,), 0, tiles)
    step_over = jax.random.randint(jax.random.fold_in(key, 15), (PERSONS,), 0, max(tiles - 1, 1))
    tile_two = (tile_one + 1 + step_over) % tiles
    first_obj = (tile_one * OBJ_DEV + jax.random.randint(jax.random.fold_in(key, 16), (PERSONS,), 0, OBJ_DEV)).astype(jnp.int32)
    second_obj = (tile_two * OBJ_DEV + jax.random.randint(jax.random.fold_in(key, 17), (PERSONS,), 0, OBJ_DEV)).astype(jnp.int32)
    top_value = 268435456 + jax.random.randint(jax.random.fold_in(key, 18), (PERSONS,), 0, 1048576)
    person_rows = jnp.arange(PERSONS, dtype=jnp.int32)
    old_one = base[person_rows, first_obj]
    base = base.at[person_rows, first_obj].set(jnp.where(tied, top_value + price[first_obj], old_one).astype(jnp.int32))
    old_two = base[person_rows, second_obj]
    base = base.at[person_rows, second_obj].set(jnp.where(tied, top_value + price[second_obj], old_two).astype(jnp.int32))
    return base.astype(jnp.int32)


def draw_assignment(key, part):
    first, again, third = jax.random.split(key, 3)
    objects_held = jax.random.permutation(first, OBJECTS)[:PERSONS].astype(jnp.int32)
    rates = jax.random.randint(again, (PERSONS // PERS_DEV,), 2, 15)
    rolls = jax.random.randint(third, (PERSONS,), 0, 16)
    unheld = rolls < jnp.repeat(rates, PERS_DEV)
    return jnp.where(unheld, -1, objects_held).astype(jnp.int32)


def setup_inputs(seed: int = 0) -> dict:
    key_list = jax.random.split(jax.random.key(seed), 5)
    benefit = draw_benefit(jax.random.fold_in(key_list[4], 71), 0)
    prices = draw_prices(jax.random.fold_in(key_list[4], 71), 0)
    assignment = draw_assignment(jax.random.fold_in(key_list[4], 71), 0)
    epsilon = jax.random.randint(key_list[3], (1,), 1, 1025).astype(jnp.int32)
    return dict(benefit=benefit, prices=prices, assignment=assignment, epsilon=epsilon)


LOWEST = -2147483647
LARGEST = 2147483647


def top_two(benefit, price):
    blocks = benefit.reshape(PERSONS // PERS_DEV, PERS_DEV, OBJECTS)
    columns = jnp.arange(OBJECTS, dtype=jnp.int32)

    def one_block(rows):
        value = rows - price[None, :]
        best = jnp.max(value, axis=1)
        target = jnp.argmax(value, axis=1).astype(jnp.int32)
        others = jnp.where(columns[None, :] == target[:, None], LOWEST, value)
        second = jnp.max(others, axis=1)
        return best, target, second

    best, target, second = lax.map(one_block, blocks)
    return best.reshape(PERSONS), target.reshape(PERSONS), second.reshape(PERSONS)


def reference(benefit, prices, assignment, epsilon):
    price = prices
    owner_of = assignment
    persons = jnp.arange(PERSONS, dtype=jnp.int32)
    for step in range(ROUNDS):
        best, target, second = top_two(benefit, price)
        free = owner_of < 0
        bid = price[target] + best - second + epsilon[0]
        slot = jnp.where(free, target, OBJECTS).astype(jnp.int32)
        top_bid = jnp.zeros((OBJECTS,), jnp.int32).at[slot].max(bid, mode="drop")
        chosen = free & (bid == top_bid[target])
        winner = jnp.full((OBJECTS,), LARGEST, jnp.int32).at[jnp.where(chosen, target, OBJECTS)].min(persons, mode="drop")
        taken = top_bid > 0
        won = free & (winner[target] == persons)
        lost = jnp.logical_not(free) & taken[jnp.clip(owner_of, 0, OBJECTS - 1)]
        owner_of = jnp.where(won, target, jnp.where(lost, -1, owner_of)).astype(jnp.int32)
        price = jnp.where(taken, top_bid, price)
    return price, owner_of
```

```python
import functools

import jax
import jax.numpy as jnp
from jax import lax
from jax.experimental import pallas as pl
from jax.experimental.pallas import tpu as pltpu
from jax.sharding import PartitionSpec as P

ROUNDS = 4
LOWEST = -2147483647
LARGEST = 2147483647
LANES = 128
MESH = pl.DeviceIdType.MESH


def top_level_sizes(pers, objs):
    return pers // LANES, objs // LANES


def kernel(
    nrow, ncol, pers, objs,
    ben_hbm, price_in, own_in, eps_ref,
    price_out, own_out,
    ben, price, owner, one, two, lane_one, buf1, buf2, buf3, tg,
    ben_sem, s1, r1, s2, r2, s3, r3,
):
    pb_n, jb_n = top_level_sizes(pers, objs)
    row, col = lax.axis_index("row"), lax.axis_index("col")
    share = ncol // pb_n
    my_block = col // share

    loads = [
        pltpu.make_async_copy(
            ben_hbm.at[pl.ds(b * LANES, LANES)], ben.at[pl.ds(b * LANES, LANES)], ben_sem.at[b]
        )
        for b in range(pb_n)
    ]
    for load in loads:
        load.start()

    barrier = pltpu.get_barrier_semaphore()
    for k in range(1, ncol):
        pl.semaphore_signal(barrier, inc=1, device_id={"col": lax.rem(col + k, ncol)}, device_id_type=MESH)
    for k in range(1, nrow):
        pl.semaphore_signal(barrier, inc=1, device_id={"row": lax.rem(row + k, nrow)}, device_id_type=MESH)
    price[...] = price_in[...]
    owner[...] = own_in[...]
    pl.semaphore_wait(barrier, ncol - 1 + nrow - 1)

    def copy1(r, k, slot):
        return pltpu.make_async_remote_copy(
            src_ref=buf1.at[r, slot], dst_ref=buf1.at[r, slot],
            send_sem=s1.at[r, k], recv_sem=r1.at[r, slot],
            device_id={"col": lax.rem(col + k, ncol)}, device_id_type=MESH)

    def copy2(r, k, slot):
        return pltpu.make_async_remote_copy(
            src_ref=buf2.at[r, slot], dst_ref=buf2.at[r, slot],
            send_sem=s2.at[r, k], recv_sem=r2.at[r, slot],
            device_id={"row": lax.rem(row + k, nrow)}, device_id_type=MESH)

    def copy3(r, k, slot):
        return pltpu.make_async_remote_copy(
            src_ref=buf3.at[r, slot], dst_ref=buf3.at[r, slot],
            send_sem=s3.at[r, k], recv_sem=r3.at[r, slot],
            device_id={"col": lax.rem(col + k, ncol)}, device_id_type=MESH)

    sub = lax.broadcasted_iota(jnp.int32, (LANES, LANES), 0)
    lane = lax.broadcasted_iota(jnp.int32, (LANES, LANES), 1)
    group = 32

    def top_two(r):
        def block(b, _):
            @pl.when(r == 0)
            def _():
                pltpu.make_async_copy(
                    ben_hbm.at[pl.ds(b * LANES, LANES)], ben.at[pl.ds(b * LANES, LANES)], ben_sem.at[b]
                ).wait()

            for g in range(LANES // group):
                rows = pl.ds(pl.multiple_of(b * LANES + g * group, group), group)
                m1 = ben[rows, :LANES] - price[0:1, :]
                m2 = jnp.full((group, LANES), LOWEST, jnp.int32)
                at = jnp.zeros((group, LANES), jnp.int32)
                for j in range(1, jb_n):
                    v = ben[rows, j * LANES:(j + 1) * LANES] - price[j:j + 1, :]
                    more = v > m1
                    m2 = jnp.maximum(m2, jnp.where(more, m1, v))
                    at = jnp.where(more, j, at)
                    m1 = jnp.where(more, v, m1)
                here = pl.ds(g * group, group)
                one[here, :] = m1
                two[here, :] = m2
                lane_one[here, :] = at
            t1 = one[...].T
            t2 = two[...].T
            where_at = lane_one[...].T * LANES + sub
            best = jnp.max(t1, axis=0, keepdims=True)
            arg = jnp.min(jnp.where(t1 == best, where_at, LARGEST), axis=0, keepdims=True)
            second = jnp.max(jnp.where(where_at == arg, t2, t1), axis=0, keepdims=True)
            buf1[r, col, 0, pl.ds(b, 1), :] = best
            buf1[r, col, 1, pl.ds(b, 1), :] = arg
            buf1[r, col, 2, pl.ds(b, 1), :] = second
            return 0

        lax.fori_loop(0, pb_n, block, 0)

    def round_body(r, _):
        top_two(r)
        for k in range(1, ncol):
            copy1(r, k, col).start()
        for k in range(1, ncol):
            copy1(r, k, lax.rem(col + k, ncol)).wait_recv()

        best = buf1[r, 0, 0]
        for s in range(1, ncol):
            best = jnp.maximum(best, buf1[r, s, 0])
        target = jnp.full((pb_n, LANES), LARGEST, jnp.int32)
        for s in range(ncol):
            target = jnp.minimum(target, jnp.where(buf1[r, s, 0] == best, buf1[r, s, 1] + s * objs, LARGEST))
        second = jnp.full((pb_n, LANES), LOWEST, jnp.int32)
        for s in range(ncol):
            second = jnp.maximum(
                second, jnp.where(buf1[r, s, 1] + s * objs == target, buf1[r, s, 2], buf1[r, s, 0]))
        gap = best - second

        @pl.when(r > 0)
        def _():
            for k in range(1, ncol):
                copy3(r - 1, k, lax.rem(col + k, ncol)).wait_recv()
            for b in range(pb_n):
                owner[b:b + 1, :] = buf3[r - 1, b * share, 0:1, :]

        free = owner[...] < 0
        bids_on = jnp.where(free, target, -1)
        tg[0] = jnp.where(free, target, owner[...])
        tg[1] = jnp.where(free, gap, -1)
        tg[2] = jnp.where(free, target - col * objs, -1)
        buf2[r, row, jb_n:jb_n + pb_n, :] = bids_on
        buf2[r, row, jb_n + pb_n:, :] = gap

        def objects(j, _):
            acc = jnp.full((LANES, LANES), -1, jnp.int32)
            ids = sub + j * LANES
            for b in range(pb_n):
                hit = tg[2, b:b + 1, :] == ids
                acc = jnp.maximum(acc, jnp.where(hit, tg[1, b:b + 1, :], -1))
            buf2[r, row, pl.ds(j, 1), :] = jnp.max(acc.T, axis=0, keepdims=True)
            return 0

        lax.fori_loop(0, jb_n, objects, 0)
        for k in range(1, nrow):
            copy2(r, k, row).start()
        for k in range(1, nrow):
            copy2(r, k, lax.rem(row + k, nrow)).wait_recv()

        top = buf2[r, 0, :jb_n, :]
        for s in range(1, nrow):
            top = jnp.maximum(top, buf2[r, s, :jb_n, :])
        price[...] = jnp.where(top >= 0, price[...] + top + eps_ref[0], price[...])

        want = jnp.broadcast_to(tg[0, pl.ds(my_block, 1), :], (LANES, LANES)).T
        mine = jnp.broadcast_to(tg[1, pl.ds(my_block, 1), :], (LANES, LANES)).T
        me = row * pers + my_block * LANES + sub
        one[...] = jnp.zeros((LANES, LANES), jnp.int32)

        def rivals(s, _):
            beaten = one[...]
            for b in range(pb_n):
                other = s * pers + b * LANES + lane
                wish = buf2[r, s, jb_n + b:jb_n + b + 1, :]
                gaps = buf2[r, s, jb_n + pb_n + b:jb_n + pb_n + b + 1, :]
                bar = jnp.where(other < me, mine - 1, mine)
                beaten = jnp.where((wish == want) & (gaps > bar), 1, beaten)
            one[...] = beaten
            return 0

        lax.fori_loop(0, nrow, rivals, 0)
        lost = jnp.max(one[...].T, axis=0, keepdims=True)
        buf3[r, col, 0:1, :] = jnp.where(lost > 0, -1, tg[0, pl.ds(my_block, 1), :])
        for k in range(1, ncol):
            copy3(r, k, col).start()
        return 0

    lax.fori_loop(0, ROUNDS, round_body, 0)

    price_out[...] = price[...]
    for k in range(1, ncol):
        copy3(ROUNDS - 1, k, lax.rem(col + k, ncol)).wait_recv()
    for b in range(pb_n):
        own_out[b:b + 1, :] = buf3[ROUNDS - 1, b * share, 0:1, :]

    def drain(r, _):
        for k in range(1, ncol):
            copy1(r, k, col).wait_send()
            copy3(r, k, col).wait_send()
        for k in range(1, nrow):
            copy2(r, k, row).wait_send()
        return 0

    lax.fori_loop(0, ROUNDS, drain, 0)


def solution(mesh):
    nrow, ncol = mesh.shape["row"], mesh.shape["col"]

    def on_device(benefit, prices, assignment, epsilon):
        pers, objs = benefit.shape
        pb_n, jb_n = top_level_sizes(pers, objs)
        assert ncol % pb_n == 0
        vmem = pl.BlockSpec(memory_space=pltpu.VMEM)
        dma = pltpu.SemaphoreType.DMA
        price, owner = pl.pallas_call(
            functools.partial(kernel, nrow, ncol, pers, objs),
            out_shape=(
                jax.ShapeDtypeStruct((jb_n, LANES), jnp.int32),
                jax.ShapeDtypeStruct((pb_n, LANES), jnp.int32),
            ),
            in_specs=[
                pl.BlockSpec(memory_space=pl.ANY), vmem, vmem,
                pl.BlockSpec(memory_space=pltpu.SMEM),
            ],
            out_specs=(vmem, vmem),
            scratch_shapes=[
                pltpu.VMEM((pers, objs), jnp.int32),
                pltpu.VMEM((jb_n, LANES), jnp.int32),
                pltpu.VMEM((pb_n, LANES), jnp.int32),
                pltpu.VMEM((LANES, LANES), jnp.int32),
                pltpu.VMEM((LANES, LANES), jnp.int32),
                pltpu.VMEM((LANES, LANES), jnp.int32),
                pltpu.VMEM((ROUNDS, ncol, 3, pb_n, LANES), jnp.int32),
                pltpu.VMEM((ROUNDS, nrow, jb_n + 2 * pb_n, LANES), jnp.int32),
                pltpu.VMEM((ROUNDS, ncol, 8, LANES), jnp.int32),
                pltpu.VMEM((3, pb_n, LANES), jnp.int32),
                dma((pb_n,)),
                dma((ROUNDS, ncol)), dma((ROUNDS, ncol)),
                dma((ROUNDS, nrow)), dma((ROUNDS, nrow)),
                dma((ROUNDS, ncol)), dma((ROUNDS, ncol)),
            ],
            compiler_params=pltpu.CompilerParams(collective_id=0, has_side_effects=True),
            name="auction",
        )(benefit, prices.reshape(jb_n, LANES), assignment.reshape(pb_n, LANES), epsilon)
        return price.reshape(objs), owner.reshape(pers)

    return jax.shard_map(
        on_device,
        mesh=mesh,
        in_specs=(P("row", "col"), P("col"), P("row"), P()),
        out_specs=(P("col"), P("row")),
        check_vma=False,
    )
```

```python
import functools

import jax
import jax.numpy as jnp
from jax import lax
from jax.experimental import pallas as pl
from jax.experimental.pallas import tpu as pltpu
from jax.sharding import PartitionSpec as P

ROUNDS = 4
LOWEST = -2147483647
LARGEST = 2147483647
LANES = 128
MESH = pl.DeviceIdType.MESH


def top_level_sizes(pers, objs):
    return pers // LANES, objs // LANES


def merge(left, right):
    b0, s0, a0 = left
    b1, s1, a1 = right
    keep = b0 >= b1
    lower = jnp.where(keep, b1, b0)
    rest = lower if s0 is None else jnp.maximum(lower, jnp.where(keep, s0, s1))
    return jnp.where(keep, b0, b1), rest, jnp.where(keep, a0, a1)


SORT8 = (
    (0, 1), (2, 3), (4, 5), (6, 7), (0, 2), (1, 3), (4, 6), (5, 7), (1, 2), (5, 6),
    (0, 4), (1, 5), (2, 6), (3, 7), (2, 4), (3, 5), (1, 2), (3, 4), (5, 6),
)


def exchanges(count):
    if count == 8:
        return SORT8
    return tuple((i, i + 1) for end in range(count - 1, 0, -1) for i in range(end))


def kernel(
    nrow, ncol, pers, objs, per_part,
    ben_hbm, price_in, own_in, eps_ref,
    price_out, own_out,
    ben, price, owner, beaten, wants, buf1, buf2, buft, buf3, tg, ranked,
    ben_sem, s1, r1, s2, r2, st, rt, s3, r3,
):
    pb_n, jb_n = top_level_sizes(pers, objs)
    parts = pb_n // per_part
    part_rows = per_part * LANES
    row, col = lax.axis_index("row"), lax.axis_index("col")
    share = ncol // pb_n
    my_block = col // share
    sub = lax.broadcasted_iota(jnp.int32, (8, LANES), 0)
    lane = lax.broadcasted_iota(jnp.int32, (8, LANES), 1)
    groups = LANES // 8

    def load(p):
        rows = pl.ds(pl.multiple_of(p * part_rows, part_rows), part_rows)
        return pltpu.make_async_copy(ben_hbm.at[rows], ben.at[rows], ben_sem.at[p])

    for p in range(parts):
        load(p).start()

    barrier = pltpu.get_barrier_semaphore()
    for k in range(1, ncol):
        pl.semaphore_signal(barrier, inc=1, device_id={"col": lax.rem(col + k, ncol)}, device_id_type=MESH)
    for k in range(1, nrow):
        pl.semaphore_signal(barrier, inc=1, device_id={"row": lax.rem(row + k, nrow)}, device_id_type=MESH)
    price[...] = price_in[...]
    owner[...] = own_in[...]
    pl.semaphore_wait(barrier, ncol - 1 + nrow - 1)

    def along_col(buf, at, send, recv, k):
        ref = buf.at[at]
        return pltpu.make_async_remote_copy(
            src_ref=ref, dst_ref=ref, send_sem=send, recv_sem=recv,
            device_id={"col": lax.rem(col + k, ncol)}, device_id_type=MESH)

    def along_row(buf, at, send, recv, k):
        ref = buf.at[at]
        return pltpu.make_async_remote_copy(
            src_ref=ref, dst_ref=ref, send_sem=send, recv_sem=recv,
            device_id={"row": lax.rem(row + k, nrow)}, device_id_type=MESH)

    def copy1(r, p, k, slot):
        return along_col(buf1, (r, p, slot, pl.ds(0, 3 * per_part)), s1.at[r, p, k], r1.at[r, p, slot], k)

    def copy2(r, k, slot):
        return along_row(buf2, (r, slot), s2.at[r, k], r2.at[r, slot], k)

    def copyt(r, k, slot):
        return along_row(buft, (r, slot), st.at[r, k], rt.at[r, slot], k)

    def copy3(r, k, slot):
        return along_col(buf3, (r, slot, pl.ds(0, 1)), s3.at[r, k], r3.at[r, slot], k)

    def row_of(ref, *at):
        return jnp.broadcast_to(ref[at], (8, LANES))

    def fold(terms, combine):
        while len(terms) > 1:
            terms = [combine(*terms[i:i + 2]) if i + 1 < len(terms) else terms[i] for i in range(0, len(terms), 2)]
        return terms[0]

    def cut(square):
        return [square[8 * g:8 * g + 8] for g in range(groups)]

    def block_top(start):
        tops = []
        for g in range(groups):
            rows = pl.ds(pl.multiple_of(start + 8 * g, 8), 8)

            def tree(lo, n):
                if n == 1:
                    return ben[rows, lo * LANES:(lo + 1) * LANES] - price[lo:lo + 1, :], None, lo
                half = n // 2
                return merge(tree(lo, half), tree(lo + half, n - half))

            m1, m2, at = tree(0, jb_n)
            tops.append((m1, m2, at * LANES + lane))
        t1, t2, ta = (cut(jnp.concatenate([t[i] for t in tops], axis=0).T) for i in range(3))

        def pick(x, y):
            (b0, s0, a0), (b1, s1_, a1) = x, y
            keep = (b0 > b1) | (b0 == b1) & (a0 < a1)
            return (
                jnp.where(keep, b0, b1),
                jnp.maximum(jnp.where(keep, b1, b0), jnp.where(keep, s0, s1_)),
                jnp.where(keep, a0, a1),
            )

        b8, s8, a8 = fold(list(zip(t1, t2, ta)), pick)
        best = jnp.max(b8, axis=0, keepdims=True)
        arg = jnp.min(jnp.where(b8 == best, a8, LARGEST), axis=0, keepdims=True)
        second = jnp.max(jnp.where(a8 == arg, s8, b8), axis=0, keepdims=True)
        return best, arg, second

    def round_body(r, _):
        def part(p, _):
            @pl.when(r == 0)
            def _():
                load(p).wait()

            for i in range(per_part):
                best, arg, second = block_top(p * part_rows + i * LANES)
                buf1[r, p, col, i:i + 1, :] = best
                buf1[r, p, col, per_part + i:per_part + i + 1, :] = arg
                buf1[r, p, col, 2 * per_part + i:2 * per_part + i + 1, :] = second
            for k in range(1, ncol):
                copy1(r, p, k, col).start()
            return 0

        lax.fori_loop(0, parts, part, 0)

        @pl.when(r > 0)
        def _():
            for k in range(1, ncol):
                copy3(r - 1, k, lax.rem(col + k, ncol)).wait_recv()
            for b in range(pb_n):
                owner[b:b + 1, :] = buf3[r - 1, b * share, 0:1, :]

        for p in range(parts):
            for k in range(1, ncol):
                copy1(r, p, k, lax.rem(col + k, ncol)).wait_recv()
            q = per_part
            bests = [buf1[r, p, s, 0:q, :] for s in range(ncol)]
            args = [buf1[r, p, s, q:2 * q, :] + s * objs for s in range(ncol)]
            best = fold(bests, jnp.maximum)
            target = fold([jnp.where(b == best, a, LARGEST) for b, a in zip(bests, args)], jnp.minimum)
            second = fold(
                [jnp.where(a == target, buf1[r, p, s, 2 * q:3 * q, :], b)
                 for s, (b, a) in enumerate(zip(bests, args))], jnp.maximum)
            here = slice(p * q, (p + 1) * q)
            held = owner[here, :]
            free = held < 0
            gap = best - second
            buft[r, row, here, :] = jnp.where(free, target, -1)
            buft[r, row, pb_n + p * q:pb_n + (p + 1) * q, :] = gap
            tg[0, here, :] = jnp.where(free, target, held)
            tg[1, here, :] = jnp.where(free, gap, -1)
        for k in range(1, nrow):
            copyt(r, k, row).start()

        pairs = []
        for b in range(pb_n):
            local = row_of(buft, r, row, slice(b, b + 1))
            pairs.append((row_of(tg, 1, slice(b, b + 1)), local - col * objs - sub))
        for i, j in exchanges(pb_n):
            (g0, d0), (g1, d1) = pairs[i], pairs[j]
            keep = g0 <= g1
            pairs[i] = (jnp.where(keep, g0, g1), jnp.where(keep, d0, d1))
            pairs[j] = (jnp.where(keep, g1, g0), jnp.where(keep, d1, d0))
        for b in range(pb_n):
            ranked[0, b], ranked[1, b] = pairs[b]

        def objects(j, _):
            gaps = [ranked[0, b] for b in range(pb_n)]
            offs = [ranked[1, b] - j * LANES for b in range(pb_n)]
            rows = []
            for g in range(groups):
                acc = jnp.full((8, LANES), -1, jnp.int32)
                for gap_b, off in zip(gaps, offs):
                    acc = jnp.where(off == 8 * g, gap_b, acc)
                rows.append(acc)
            top = fold(cut(jnp.concatenate(rows, axis=0).T), jnp.maximum)
            buf2[r, row, pl.ds(j, 1), :] = jnp.max(top, axis=0, keepdims=True)
            return 0

        lax.fori_loop(0, jb_n, objects, 0, unroll=2)
        for k in range(1, nrow):
            copy2(r, k, row).start()

        wants[0] = jnp.broadcast_to(tg[0, pl.ds(my_block, 1), :], (LANES, LANES)).T
        wants[1] = jnp.broadcast_to(tg[1, pl.ds(my_block, 1), :], (LANES, LANES)).T
        wish = row_of(buft, r, row, pl.ds(my_block, 1))
        gaps = row_of(buft, r, row, pl.ds(pb_n + my_block, 1))
        for g in range(groups):
            at = slice(8 * g, 8 * g + 8)
            tie = (wish == wants[0, at]) & (gaps == wants[1, at]) & (lane < sub + 8 * g)
            beaten[at, :] = jnp.where(tie, 1, 0)

        def rivals(i, _):
            s = lax.rem(row + i, nrow)

            @pl.when(i > 0)
            def _():
                copyt(r, nrow - i, s).wait_recv()

            wishes, lifts = [], []
            for b in range(pb_n):
                ahead = s * pers + b * LANES < row * pers + my_block * LANES
                wishes.append(row_of(buft, r, s, slice(b, b + 1)))
                lifts.append(row_of(buft, r, s, slice(pb_n + b, pb_n + b + 1)) + jnp.where(ahead, 1, 0))
            for g in range(groups):
                at = slice(8 * g, 8 * g + 8)
                want, mine, acc = wants[0, at], wants[1, at], beaten[at, :]
                for w, lift in zip(wishes, lifts):
                    acc = jnp.where((w == want) & (lift > mine), 1, acc)
                beaten[at, :] = acc
            return 0

        lax.fori_loop(0, nrow, rivals, 0)
        lost = jnp.max(fold(cut(beaten[...].T), jnp.bitwise_or), axis=0, keepdims=True)
        buf3[r, col, 0:1, :] = jnp.where(lost > 0, -1, tg[0, pl.ds(my_block, 1), :])
        for k in range(1, ncol):
            copy3(r, k, col).start()

        for k in range(1, nrow):
            copy2(r, k, lax.rem(row + k, nrow)).wait_recv()
        top = fold([buf2[r, s] for s in range(nrow)], jnp.maximum)
        price[...] = jnp.where(top >= 0, price[...] + top + eps_ref[0], price[...])
        return 0

    lax.fori_loop(0, ROUNDS, round_body, 0)

    price_out[...] = price[...]
    for k in range(1, ncol):
        copy3(ROUNDS - 1, k, lax.rem(col + k, ncol)).wait_recv()
    for b in range(pb_n):
        own_out[b:b + 1, :] = buf3[ROUNDS - 1, b * share, 0:1, :]

    def drain(r, _):
        for k in range(1, ncol):
            for p in range(parts):
                copy1(r, p, k, col).wait_send()
            copy3(r, k, col).wait_send()
        for k in range(1, nrow):
            copy2(r, k, row).wait_send()
            copyt(r, k, row).wait_send()
        return 0

    lax.fori_loop(0, ROUNDS, drain, 0)


def solution(mesh):
    nrow, ncol = mesh.shape["row"], mesh.shape["col"]

    def on_device(benefit, prices, assignment, epsilon):
        pers, objs = benefit.shape
        pb_n, jb_n = top_level_sizes(pers, objs)
        assert ncol % pb_n == 0
        per_part = 2
        parts = pb_n // per_part
        vmem = pl.BlockSpec(memory_space=pltpu.VMEM)
        dma = pltpu.SemaphoreType.DMA
        price, owner = pl.pallas_call(
            functools.partial(kernel, nrow, ncol, pers, objs, per_part),
            out_shape=(
                jax.ShapeDtypeStruct((jb_n, LANES), jnp.int32),
                jax.ShapeDtypeStruct((pb_n, LANES), jnp.int32),
            ),
            in_specs=[
                pl.BlockSpec(memory_space=pl.ANY), vmem, vmem,
                pl.BlockSpec(memory_space=pltpu.SMEM),
            ],
            out_specs=(vmem, vmem),
            scratch_shapes=[
                pltpu.VMEM((pers, objs), jnp.int32),
                pltpu.VMEM((jb_n, LANES), jnp.int32),
                pltpu.VMEM((pb_n, LANES), jnp.int32),
                pltpu.VMEM((LANES, LANES), jnp.int32),
                pltpu.VMEM((2, LANES, LANES), jnp.int32),
                pltpu.VMEM((ROUNDS, parts, ncol, 8, LANES), jnp.int32),
                pltpu.VMEM((ROUNDS, nrow, jb_n, LANES), jnp.int32),
                pltpu.VMEM((ROUNDS, nrow, 2 * pb_n, LANES), jnp.int32),
                pltpu.VMEM((ROUNDS, ncol, 8, LANES), jnp.int32),
                pltpu.VMEM((2, pb_n, LANES), jnp.int32),
                pltpu.VMEM((2, pb_n, 8, LANES), jnp.int32),
                dma((parts,)),
                dma((ROUNDS, parts, ncol)), dma((ROUNDS, parts, ncol)),
                dma((ROUNDS, nrow)), dma((ROUNDS, nrow)),
                dma((ROUNDS, nrow)), dma((ROUNDS, nrow)),
                dma((ROUNDS, ncol)), dma((ROUNDS, ncol)),
            ],
            compiler_params=pltpu.CompilerParams(collective_id=0, has_side_effects=True),
            name="auction",
        )(benefit, prices.reshape(jb_n, LANES), assignment.reshape(pb_n, LANES), epsilon)
        return price.reshape(objs), owner.reshape(pers)

    return jax.shard_map(
        on_device,
        mesh=mesh,
        in_specs=(P("row", "col"), P("col"), P("row"), P()),
        out_specs=(P("col"), P("row")),
        check_vma=False,
    )
```

```python
import functools

import jax
import jax.numpy as jnp
from jax import lax
from jax.experimental import pallas as pl
from jax.experimental.pallas import tpu as pltpu
from jax.sharding import PartitionSpec as P

ROUNDS = 4
LOWEST = -2147483647
LARGEST = 2147483647
LANES = 128
MESH = pl.DeviceIdType.MESH


def top_level_sizes(pers, objs):
    return pers // LANES, objs // LANES


def merge(left, right):
    b0, s0, a0 = left
    b1, s1, a1 = right
    keep = b0 >= b1
    lower = jnp.where(keep, b1, b0)
    rest = lower if s0 is None else jnp.maximum(lower, jnp.where(keep, s0, s1))
    return jnp.where(keep, b0, b1), rest, jnp.where(keep, a0, a1)


SORT8 = (
    (0, 1), (2, 3), (4, 5), (6, 7), (0, 2), (1, 3), (4, 6), (5, 7), (1, 2), (5, 6),
    (0, 4), (1, 5), (2, 6), (3, 7), (2, 4), (3, 5), (1, 2), (3, 4), (5, 6),
)


def exchanges(count):
    if count == 8:
        return SORT8
    return tuple((i, i + 1) for end in range(count - 1, 0, -1) for i in range(end))


def kernel(
    nrow, ncol, pers, objs, per_part,
    ben_hbm, price_in, own_in, eps_ref,
    price_out, own_out,
    ben, price, owner, beaten, wants, buf1, buf2, buft, buf3, tg, ranked,
    ben_sem, s1, r1, s2, r2, st, rt, s3, r3,
):
    pb_n, jb_n = top_level_sizes(pers, objs)
    parts = pb_n // per_part
    part_rows = per_part * LANES
    row, col = lax.axis_index("row"), lax.axis_index("col")
    share = ncol // pb_n
    my_block = col // share
    sub = lax.broadcasted_iota(jnp.int32, (8, LANES), 0)
    lane = lax.broadcasted_iota(jnp.int32, (8, LANES), 1)
    groups = LANES // 8

    def load(p):
        rows = pl.ds(pl.multiple_of(p * part_rows, part_rows), part_rows)
        return pltpu.make_async_copy(ben_hbm.at[rows], ben.at[rows], ben_sem.at[p])

    for p in range(parts):
        load(p).start()

    barrier = pltpu.get_barrier_semaphore()
    for k in range(1, ncol):
        pl.semaphore_signal(barrier, inc=1, device_id={"col": lax.rem(col + k, ncol)}, device_id_type=MESH)
    for k in range(1, nrow):
        pl.semaphore_signal(barrier, inc=1, device_id={"row": lax.rem(row + k, nrow)}, device_id_type=MESH)
    price[...] = price_in[...]
    owner[...] = own_in[...]

    def along_col(buf, at, send, recv, k):
        ref = buf.at[at]
        return pltpu.make_async_remote_copy(
            src_ref=ref, dst_ref=ref, send_sem=send, recv_sem=recv,
            device_id={"col": lax.rem(col + k, ncol)}, device_id_type=MESH)

    def along_row(buf, at, send, recv, k):
        ref = buf.at[at]
        return pltpu.make_async_remote_copy(
            src_ref=ref, dst_ref=ref, send_sem=send, recv_sem=recv,
            device_id={"row": lax.rem(row + k, nrow)}, device_id_type=MESH)

    def copy1(r, p, k, slot):
        return along_col(buf1, (r, p, slot, pl.ds(0, 3 * per_part)), s1.at[r, p, k], r1.at[r, p, slot], k)

    def copy2(r, k, slot):
        return along_row(buf2, (r, slot), s2.at[r, k], r2.at[r, slot], k)

    def copyt(r, k, slot):
        return along_row(buft, (r, slot), st.at[r, k], rt.at[r, slot], k)

    def copy3(r, k, slot):
        return along_col(buf3, (r, slot, pl.ds(0, 1)), s3.at[r, k], r3.at[r, slot], k)

    def row_of(ref, *at):
        return jnp.broadcast_to(ref[at], (8, LANES))

    def fold(terms, combine):
        while len(terms) > 1:
            terms = [combine(*terms[i:i + 2]) if i + 1 < len(terms) else terms[i] for i in range(0, len(terms), 2)]
        return terms[0]

    def cut(square):
        return [square[8 * g:8 * g + 8] for g in range(groups)]

    def block_top(start):
        tops = []
        for g in range(groups):
            rows = pl.ds(pl.multiple_of(start + 8 * g, 8), 8)

            def tree(lo, n):
                if n == 1:
                    return ben[rows, lo * LANES:(lo + 1) * LANES] - price[lo:lo + 1, :], None, lo
                half = n // 2
                return merge(tree(lo, half), tree(lo + half, n - half))

            m1, m2, at = tree(0, jb_n)
            tops.append((m1, m2, at * LANES + lane))
        t1, t2, ta = (cut(jnp.concatenate([t[i] for t in tops], axis=0).T) for i in range(3))

        def pick(x, y):
            (b0, s0, a0), (b1, s1_, a1) = x, y
            keep = (b0 > b1) | (b0 == b1) & (a0 < a1)
            return (
                jnp.where(keep, b0, b1),
                jnp.maximum(jnp.where(keep, b1, b0), jnp.where(keep, s0, s1_)),
                jnp.where(keep, a0, a1),
            )

        b8, s8, a8 = fold(list(zip(t1, t2, ta)), pick)
        best = jnp.max(b8, axis=0, keepdims=True)
        arg = jnp.min(jnp.where(b8 == best, a8, LARGEST), axis=0, keepdims=True)
        second = jnp.max(jnp.where(a8 == arg, s8, b8), axis=0, keepdims=True)
        return best, arg, second

    def round_body(r, _):
        def part(p, _):
            @pl.when(r == 0)
            def _():
                load(p).wait()

            for i in range(per_part):
                best, arg, second = block_top(p * part_rows + i * LANES)
                buf1[r, p, col, i:i + 1, :] = best
                buf1[r, p, col, per_part + i:per_part + i + 1, :] = arg
                buf1[r, p, col, 2 * per_part + i:2 * per_part + i + 1, :] = second

            @pl.when((r == 0) & (p == 0))
            def _():
                pl.semaphore_wait(barrier, ncol - 1 + nrow - 1)

            for k in range(1, ncol):
                copy1(r, p, k, col).start()
            return 0

        lax.fori_loop(0, parts, part, 0)

        @pl.when(r > 0)
        def _():
            for k in range(1, ncol):
                copy3(r - 1, k, lax.rem(col + k, ncol)).wait_recv()
            for b in range(pb_n):
                owner[b:b + 1, :] = buf3[r - 1, b * share, 0:1, :]

        for p in range(parts):
            for k in range(1, ncol):
                copy1(r, p, k, lax.rem(col + k, ncol)).wait_recv()
            q = per_part
            bests = [buf1[r, p, s, 0:q, :] for s in range(ncol)]
            args = [buf1[r, p, s, q:2 * q, :] + s * objs for s in range(ncol)]
            best = fold(bests, jnp.maximum)
            target = fold([jnp.where(b == best, a, LARGEST) for b, a in zip(bests, args)], jnp.minimum)
            second = fold(
                [jnp.where(a == target, buf1[r, p, s, 2 * q:3 * q, :], b)
                 for s, (b, a) in enumerate(zip(bests, args))], jnp.maximum)
            here = slice(p * q, (p + 1) * q)
            held = owner[here, :]
            free = held < 0
            gap = best - second
            buft[r, row, here, :] = jnp.where(free, target, -1)
            buft[r, row, pb_n + p * q:pb_n + (p + 1) * q, :] = gap
            tg[0, here, :] = jnp.where(free, target, held)
            tg[1, here, :] = jnp.where(free, gap, -1)
        for k in range(1, nrow):
            copyt(r, k, row).start()

        pairs = []
        for b in range(pb_n):
            local = row_of(buft, r, row, slice(b, b + 1))
            pairs.append((row_of(tg, 1, slice(b, b + 1)), local - col * objs - sub))
        for i, j in exchanges(pb_n):
            (g0, d0), (g1, d1) = pairs[i], pairs[j]
            keep = g0 <= g1
            pairs[i] = (jnp.where(keep, g0, g1), jnp.where(keep, d0, d1))
            pairs[j] = (jnp.where(keep, g1, g0), jnp.where(keep, d1, d0))
        for b in range(pb_n):
            ranked[0, b], ranked[1, b] = pairs[b]

        def objects(j, _):
            gaps = [ranked[0, b] for b in range(pb_n)]
            offs = [ranked[1, b] - j * LANES for b in range(pb_n)]
            rows = []
            for g in range(groups):
                acc = jnp.full((8, LANES), -1, jnp.int32)
                for gap_b, off in zip(gaps, offs):
                    acc = jnp.where(off == 8 * g, gap_b, acc)
                rows.append(acc)
            top = fold(cut(jnp.concatenate(rows, axis=0).T), jnp.maximum)
            buf2[r, row, pl.ds(j, 1), :] = jnp.max(top, axis=0, keepdims=True)
            return 0

        lax.fori_loop(0, jb_n, objects, 0, unroll=2)
        for k in range(1, nrow):
            copy2(r, k, row).start()

        wants[0] = jnp.broadcast_to(tg[0, pl.ds(my_block, 1), :], (LANES, LANES)).T
        wants[1] = jnp.broadcast_to(tg[1, pl.ds(my_block, 1), :], (LANES, LANES)).T
        wish = row_of(buft, r, row, pl.ds(my_block, 1))
        gaps = row_of(buft, r, row, pl.ds(pb_n + my_block, 1))
        for g in range(groups):
            at = slice(8 * g, 8 * g + 8)
            tie = (wish == wants[0, at]) & (gaps == wants[1, at]) & (lane < sub + 8 * g)
            beaten[at, :] = jnp.where(tie, 1, 0)

        def rivals(i, _):
            s = lax.rem(row + i, nrow)

            @pl.when(i > 0)
            def _():
                copyt(r, nrow - i, s).wait_recv()

            wishes, lifts = [], []
            for b in range(pb_n):
                ahead = s * pers + b * LANES < row * pers + my_block * LANES
                wishes.append(row_of(buft, r, s, slice(b, b + 1)))
                lifts.append(row_of(buft, r, s, slice(pb_n + b, pb_n + b + 1)) + jnp.where(ahead, 1, 0))
            for g in range(groups):
                at = slice(8 * g, 8 * g + 8)
                want, mine, acc = wants[0, at], wants[1, at], beaten[at, :]
                for w, lift in zip(wishes, lifts):
                    acc = jnp.where((w == want) & (lift > mine), 1, acc)
                beaten[at, :] = acc
            return 0

        lax.fori_loop(0, nrow, rivals, 0)
        lost = jnp.max(fold(cut(beaten[...].T), jnp.bitwise_or), axis=0, keepdims=True)
        buf3[r, col, 0:1, :] = jnp.where(lost > 0, -1, tg[0, pl.ds(my_block, 1), :])
        for k in range(1, ncol):
            copy3(r, k, col).start()

        for k in range(1, nrow):
            copy2(r, k, lax.rem(row + k, nrow)).wait_recv()
        top = fold([buf2[r, s] for s in range(nrow)], jnp.maximum)
        price[...] = jnp.where(top >= 0, price[...] + top + eps_ref[0], price[...])
        return 0

    lax.fori_loop(0, ROUNDS, round_body, 0)

    price_out[...] = price[...]
    for k in range(1, ncol):
        copy3(ROUNDS - 1, k, lax.rem(col + k, ncol)).wait_recv()
    for b in range(pb_n):
        own_out[b:b + 1, :] = buf3[ROUNDS - 1, b * share, 0:1, :]

    def drain(r, _):
        for k in range(1, ncol):
            for p in range(parts):
                copy1(r, p, k, col).wait_send()
            copy3(r, k, col).wait_send()
        for k in range(1, nrow):
            copy2(r, k, row).wait_send()
            copyt(r, k, row).wait_send()
        return 0

    lax.fori_loop(0, ROUNDS, drain, 0)


def solution(mesh):
    nrow, ncol = mesh.shape["row"], mesh.shape["col"]

    def on_device(benefit, prices, assignment, epsilon):
        pers, objs = benefit.shape
        pb_n, jb_n = top_level_sizes(pers, objs)
        assert ncol % pb_n == 0
        per_part = 4
        parts = pb_n // per_part
        vmem = pl.BlockSpec(memory_space=pltpu.VMEM)
        dma = pltpu.SemaphoreType.DMA
        price, owner = pl.pallas_call(
            functools.partial(kernel, nrow, ncol, pers, objs, per_part),
            out_shape=(
                jax.ShapeDtypeStruct((jb_n, LANES), jnp.int32),
                jax.ShapeDtypeStruct((pb_n, LANES), jnp.int32),
            ),
            in_specs=[
                pl.BlockSpec(memory_space=pl.ANY), vmem, vmem,
                pl.BlockSpec(memory_space=pltpu.SMEM),
            ],
            out_specs=(vmem, vmem),
            scratch_shapes=[
                pltpu.VMEM((pers, objs), jnp.int32),
                pltpu.VMEM((jb_n, LANES), jnp.int32),
                pltpu.VMEM((pb_n, LANES), jnp.int32),
                pltpu.VMEM((LANES, LANES), jnp.int32),
                pltpu.VMEM((2, LANES, LANES), jnp.int32),
                pltpu.VMEM((ROUNDS, parts, ncol, 16, LANES), jnp.int32),
                pltpu.VMEM((ROUNDS, nrow, jb_n, LANES), jnp.int32),
                pltpu.VMEM((ROUNDS, nrow, 2 * pb_n, LANES), jnp.int32),
                pltpu.VMEM((ROUNDS, ncol, 8, LANES), jnp.int32),
                pltpu.VMEM((2, pb_n, LANES), jnp.int32),
                pltpu.VMEM((2, pb_n, 8, LANES), jnp.int32),
                dma((parts,)),
                dma((ROUNDS, parts, ncol)), dma((ROUNDS, parts, ncol)),
                dma((ROUNDS, nrow)), dma((ROUNDS, nrow)),
                dma((ROUNDS, nrow)), dma((ROUNDS, nrow)),
                dma((ROUNDS, ncol)), dma((ROUNDS, ncol)),
            ],
            compiler_params=pltpu.CompilerParams(collective_id=0, has_side_effects=True),
            name="auction",
        )(benefit, prices.reshape(jb_n, LANES), assignment.reshape(pb_n, LANES), epsilon)
        return price.reshape(objs), owner.reshape(pers)

    return jax.shard_map(
        on_device,
        mesh=mesh,
        in_specs=(P("row", "col"), P("col"), P("row"), P()),
        out_specs=(P("col"), P("row")),
        check_vma=False,
    )
```
